256 devices in a mesh: outer: 8 (over x, y_hi), dp: 32 (over y_lo, z, core).
Axes of the slice: x: 4, y: 4 (y_hi: 2, y_lo: 2; y = y_hi * 2 + y_lo), z: 8, core: 2. Of those that a mesh axis runs over, the one named last changes fastest.
Arguments:
- fast_weights: float32 [8, 4096, 2048], P('outer', 'dp'), may hold values from -6 to 6
- slow_weights: float32 [4096, 2048], P('dp', 'outer'), may hold values from -6 to 6
- momentum: float32 [4096, 2048], P('dp', 'outer'), may hold values from -3 to 3
- tokens: bfloat16 [196608, 4096], P(('outer', 'dp')), may hold values from -6 to 6
- norm_gain: float32 [4096], replicated, may hold values from 0.1 to 1.9
Outputs:
- slow_next: float32 [4096, 2048], P('dp', 'outer')
- momentum_next: float32 [4096, 2048], P('dp', 'outer')
- fast_next: float32 [4096, 2048], P('dp')
- key_values: bfloat16 [196608, 2048], P(('outer', 'dp'))
The draws below stay inside these ranges and needn't reach their ends.
All inputs are finite; a program needn't handle non-finite values.
Results may differ from the reference program's by a relative error of at most 0.0057.
Values may be sent and summed in bfloat16 or wider, within the bound.
A program may use at most 128 MiB of HBM per device.

```python
import jax
import jax.numpy as jnp
from jax import lax

D = 4096
TOK_DEV = 768
COLS = 2048
PODS = 8
TOKENS = 196608
N_OUTER = 8


def strengthened(values, stream_key, source, target, parts, factor):
    def block_of(axis_at):
        return (jnp.arange(values.shape[axis_at]) // (values.shape[axis_at] // parts)).reshape((-1,) + (1,) * (values.ndim - 1 - axis_at))

    first = jax.random.permutation(stream_key, parts)[block_of(target)]
    far = (block_of(target) + parts // 2) % parts
    return jnp.where((block_of(source) == first) | (block_of(source) == far), factor * values, values)


def steps_of(rng, shape, cuts, least, high):
    loudness = 1.0
    for axis_at, blocks in cuts:
        steps = jax.random.uniform(jax.random.fold_in(jax.random.fold_in(rng, 6), axis_at), (blocks,), jnp.float32, least / len(cuts), high / len(cuts))
        loudness = loudness * jnp.repeat(jnp.exp(steps), shape[axis_at] // blocks).reshape((-1,) + (1,) * (len(shape) - 1 - axis_at))
    return loudness


def normal_values(rng, shape, width, limit, shards=(), kind=jnp.bfloat16):
    factor_of = steps_of(rng, shape, shards, -0.22, 0.18) if shards else 1.0
    entries = jax.random.normal(rng, shape, jnp.float32) * width * factor_of
    return jnp.minimum(jnp.maximum(entries, -limit), limit).astype(kind)


def noise_with(rng, dims, width, reach, split, heavy, held_as=jnp.bfloat16):
    result = width * jax.random.normal(rng, dims, jnp.float32)
    if split:
        result = result * steps_of(rng, dims, split, -0.22, 0.18)
    return jnp.clip(strengthened(result, jax.random.fold_in(rng, 3), *heavy), -reach, reach).astype(held_as)


def setup_inputs(seed: int = 0) -> dict:
    splits = jax.random.split(jax.random.key(seed), 6)
    fast_weights = noise_with(splits[0], (PODS, D, COLS), 1.0, 6.0, ((0, 8), (1, 32)), (0, 2, 8, 2.0), jnp.float32)
    slow_weights = normal_values(splits[1], (D, COLS), 1.0, 6.0, ((0, 32), (1, 8)), jnp.float32)
    momentum = normal_values(splits[2], (D, COLS), 0.5, 3.0, ((0, 32), (1, 8)), jnp.float32)
    tokens = normal_values(splits[3], (TOKENS, D), 1.0, 6.0, ((0, 256),))
    norm_gain = jnp.clip(1.0 + 0.18 * jax.random.normal(splits[4], (D,), jnp.float32), 0.1, 1.9)
    return dict(fast_weights=fast_weights, slow_weights=slow_weights, momentum=momentum, tokens=tokens, norm_gain=norm_gain)


OUTER_LR = 0.7
MOMENTUM_COEF = 0.9
EPSILON = 1e-05

def reference(fast_weights, slow_weights, momentum, tokens, norm_gain):
    outer_grad = lax.optimization_barrier(jnp.sum(slow_weights[None] - fast_weights, axis=0)) / N_OUTER
    momentum_next = MOMENTUM_COEF * momentum + outer_grad
    slow_next = slow_weights - OUTER_LR * (outer_grad + MOMENTUM_COEF * momentum_next)
    fast_next = slow_next
    weights_rounded = slow_next.astype(jnp.bfloat16).astype(jnp.float32)
    blocks = tokens.reshape(TOKENS // TOK_DEV, TOK_DEV, D)

    def project(block):
        values = block.astype(jnp.float32)
        meansq = lax.optimization_barrier(jnp.mean(values * values, axis=-1, keepdims=True))
        normed = (values * lax.rsqrt(meansq + EPSILON) * norm_gain).astype(jnp.bfloat16)
        product = jnp.dot(normed.astype(jnp.float32), weights_rounded, preferred_element_type=jnp.float32)
        return (product * D ** (-0.5)).astype(jnp.bfloat16)
    key_values = lax.map(project, blocks).reshape(TOKENS, COLS)
    return (slow_next, momentum_next, fast_next, key_values)
```

```python
import heapq

import jax
import jax.numpy as jnp
from jax import lax
from jax.experimental import pallas as pl
from jax.experimental.pallas import tpu as pltpu
from jax.sharding import PartitionSpec as P

OUTER_LR = 0.7
MOMENTUM_COEF = 0.9
EPSILON = 1e-05
MESH = pl.DeviceIdType.MESH

NX, NY, NZ = 4, 4, 8
SIZES = dict(x=NX, y=NY, z=NZ)
WAVES = 2
LANES = 128
COLOURS = (
    (("x", "y", "z"), (0, 48), (0, 48)),
    (("z", "y", "x"), (48, 96), (48, 80)),
    (("z", "x", "y"), (96, 128), (80, 128)),
)
LINK = 45.5
HOP, FURTHER = 1.9, 0.75
READY = (0.0, 3.5)


def spans(order, wave, colour):
    lo, hi = COLOURS[colour][1 + wave]
    return hi - lo


class Piece:
    def __init__(self, wave, colour, where):
        self.wave, self.colour, self.where = wave, colour, dict(where)

    def moved(self, axis, step):
        where = dict(self.where)
        where[axis] = (where[axis] - step) % SIZES[axis]
        return Piece(self.wave, self.colour, where)

    def cut(self, axis, half):
        where = dict(self.where)
        lo, hi = where[axis]
        mid = (lo + hi) // 2
        where[axis] = (lo, mid) if half == 0 else (mid, hi)
        return Piece(self.wave, self.colour, where)

    def key(self):
        return (self.wave, self.colour, tuple(sorted(self.where.items())))

    def kib(self):
        tiles = 1
        for span in self.where.values():
            if isinstance(span, tuple):
                tiles *= span[1] - span[0]
        return tiles * spans(None, self.wave, self.colour) * LANES * 2 / 1024


def ring_steps(size):
    far = size // 2
    steps = []
    for k in range(far):
        half = (0, 1) if k == far - 1 else (None, None)
        steps.append(((1, (-k) % size, half[0]), (-1, k % size, half[1])))
    return steps


def make_plan():
    free, heap, order, serial = {}, [], [], [0]
    have, followers = {}, {}

    def send(now, actions, piece, axis, step, phase):
        kib = piece.kib()
        hops = abs(step)
        link = (axis, step > 0)
        begin = max(now, free.get(link, 0.0))
        free[link] = begin + kib * hops / LINK
        arrive = begin + kib / LINK + HOP + FURTHER * (hops - 1)
        got = piece.moved(axis, step)
        index = serial[0]
        serial[0] += 1
        actions.append((piece, axis, step, phase, index))
        heapq.heappush(heap, (arrive, index, got, axis, phase, step))

    def spread(now, actions, base, axis, phase, offset, halves_axis, done_from):
        for pair in ring_steps(SIZES[axis]):
            for direction, held, half in pair:
                if held != offset:
                    continue
                if offset != 0 and done_from != direction:
                    continue
                piece = base if half is None else base.cut(halves_axis, half)
                send(now, actions, piece, axis, direction, phase)

    starts = []
    for wave in range(WAVES):
        heapq.heappush(heap, (READY[wave], -1 - wave, None, None, 0, wave))
    arrived = {}
    while heap:
        now, index, got, axis, phase, step = heapq.heappop(heap)
        actions, local = [], []
        if phase == 0:
            wave = step
            for colour, (axes, *_r) in enumerate(COLOURS):
                own = Piece(wave, colour, dict(x=0, y=0, z=0))
                a = axes[0]
                size = SIZES[a]
                for distance in range(1, size // 2 + 1):
                    for sign in (1, -1):
                        if distance == size // 2 and sign == -1:
                            continue
                        send(now, actions, own, a, sign * distance, 1)
            order.append((now, "ready", wave, None, actions, local, None))
            continue
        wave, colour = got.wave, got.colour
        a, b, c = COLOURS[colour][0]
        if phase == 1:
            tag = (wave, colour, 1)
            arrived[tag] = arrived.get(tag, 0) + 1
            if arrived[tag] == SIZES[a] - 1:
                where = {a: (0, SIZES[a]), b: 0, c: 0}
                line = Piece(wave, colour, where)
                spread(now, actions, line, b, 2, 0, a, None)
                spread(now, actions, line, c, 3, 0, a, None)
                local.append(line)
        elif phase == 2:
            offset = got.where[b]
            span = got.where[a]
            whole = span == (0, SIZES[a])
            if whole:
                spread(now, actions, got, b, 2, offset, a, step)
            full = Piece(wave, colour, {**got.where, a: (0, SIZES[a])})
            tag = full.key()
            arrived[tag] = arrived.get(tag, 0) + (2 if whole else 1)
            if arrived[tag] == 2:
                spread(now, actions, full, c, 3, 0, a, None)
                local.append(full)
        else:
            if got.where[a] == (0, SIZES[a]):
                spread(now, actions, got, c, 3, got.where[c], a, step)
            local.append(got)
        order.append((now, "recv", wave, got, actions, local, index))
    return order, serial[0]


PLAN, COPIES = make_plan()


def kernel(fast_in, slow_in, moment_in, tokens_in, gain_in,
           slow_out, moment_out, fast_out, kv_out,
           tiles, fast, outgoing, incoming, slow, moment, tokens, gain, slow_new, moment_new, fast_new, total, product,
           load_sem, store_sem, rs_send, rs_recv, ag_send, ag_recv, pair_send, pair_recv):
    outer, dp = lax.axis_index("outer"), lax.axis_index("dp")
    x, yh = outer // 2, outer % 2
    yl, z, core = dp // 16, (dp // 2) % NZ, dp % 2
    y = yh * 2 + yl
    here = dict(x=x, y=y, z=z)
    other = 1 - core

    def device(px, py, pz, pc):
        return (px * 2 + py // 2, (py % 2) * 16 + pz * 2 + pc)

    def beside(axis, step):
        at = dict(here)
        at[axis] = lax.rem(at[axis] + (step % SIZES[axis]), SIZES[axis])
        return device(at["x"], at["y"], at["z"], core)

    partner = device(x, y, z, other)

    loads = [
        pltpu.make_async_copy(fast_in.at[0], fast, load_sem.at[0]),
        pltpu.make_async_copy(slow_in, slow, load_sem.at[1]),
        pltpu.make_async_copy(moment_in, moment, load_sem.at[2]),
        pltpu.make_async_copy(gain_in, gain, load_sem.at[3]),
        pltpu.make_async_copy(tokens_in, tokens, load_sem.at[4]),
    ]
    for load in loads:
        load.start()

    peers = []
    for dx in range(NX):
        for dy in (0, 2):
            if dx or dy:
                peers.append(device(lax.rem(x + dx, NX), lax.rem(y + dy, NY), z, core))
    greet = list(peers) + [partner, beside("y", 1), beside("y", -1)] + [beside("z", s) for s in range(1, NZ)]
    barrier = pltpu.get_barrier_semaphore()
    for peer in greet:
        pl.semaphore_signal(barrier, inc=1, device_id=peer, device_id_type=MESH)

    loads[0].wait()
    for wave in range(WAVES):
        for o in range(NX * 2):
            outgoing[wave, o] = fast[:, o * 256 + wave * LANES:o * 256 + (wave + 1) * LANES].astype(jnp.bfloat16)
    loads[1].wait()
    loads[2].wait()
    loads[3].wait()
    pl.semaphore_wait(barrier, len(greet))

    for wave in range(WAVES):
        for index, peer in enumerate(peers):
            pltpu.make_async_remote_copy(
                src_ref=outgoing.at[wave, peer[0]], dst_ref=incoming.at[wave, outer],
                send_sem=rs_send.at[wave], recv_sem=rs_recv.at[wave], device_id=peer, device_id_type=MESH).start()

    def norm_rows(first, count):
        @pl.loop(first, first + count)
        def _(i):
            rows = pl.ds(i * 16, 16)
            values = tokens[rows, :].astype(jnp.float32)
            meansq = jnp.mean(values * values, axis=-1, keepdims=True)
            tokens[rows, :] = (values * lax.rsqrt(meansq + EPSILON) * gain[...]).astype(jnp.bfloat16)

    def rs_wait(wave):
        landed = incoming.at[wave, 0:7]
        pltpu.make_async_remote_copy(
            src_ref=landed, dst_ref=landed, send_sem=rs_send.at[wave], recv_sem=rs_recv.at[wave],
            device_id=partner, device_id_type=MESH).wait_recv()

    def update(wave):
        cols = slice(wave * LANES, (wave + 1) * LANES)
        summed = fast[:, pl.ds(pl.multiple_of(outer * 256 + wave * LANES, LANES), LANES)]
        for k in range(1, NX * 2):
            summed = summed + incoming[wave, lax.rem(outer + k, NX * 2)].astype(jnp.float32)
        part = slow[:, cols]
        outer_grad = part - summed / (NX * 2)
        moment_next = MOMENTUM_COEF * moment[:, cols] + outer_grad
        slow_next = part - OUTER_LR * (outer_grad + MOMENTUM_COEF * moment_next)
        tiles[wave, x, y, z, core] = slow_next.astype(jnp.bfloat16)
        slow_new[:, cols] = slow_next
        moment_new[:, cols] = moment_next

    def slice_of(piece):
        lo, hi = COLOURS[piece.colour][1 + piece.wave]
        index = [piece.wave]
        for axis in ("x", "y", "z"):
            span = piece.where[axis]
            if isinstance(span, tuple):
                index.append(slice(span[0], span[1]))
            else:
                index.append(lax.rem(here[axis] + span, SIZES[axis]) if span else here[axis])
        return tiles.at[(*index, core, slice(lo, hi), slice(None))]

    def ag_copy(piece, axis, step, phase, index):
        ref = slice_of(piece)
        return pltpu.make_async_remote_copy(
            src_ref=ref, dst_ref=ref, send_sem=ag_send.at[piece.wave, piece.colour, phase - 1], recv_sem=ag_recv.at[index],
            device_id=beside(axis, step), device_id_type=MESH)

    def pair_copy(ref, wave):
        return pltpu.make_async_remote_copy(
            src_ref=ref, dst_ref=ref, send_sem=pair_send.at[wave], recv_sem=pair_recv.at[wave],
            device_id=partner, device_id_type=MESH)

    def matmul(wave, px, part):
        yl_part, zs = part // 2, slice((part % 2) * 4, (part % 2) * 4 + 4)
        left = tiles[wave, px, yl_part, zs].reshape(1024, LANES)
        right = tiles[wave, px, 2 + yl_part, zs].reshape(1024, LANES)
        weights = jnp.concatenate([left, right], axis=1)

        @pl.loop(0, 3)
        def _(m):
            rows = pl.ds(m * 256, 256)
            value = jnp.dot(tokens[rows, part * 1024:(part + 1) * 1024], weights, preferred_element_type=jnp.float32)
            if part == 0:
                total[rows, :] = value
            elif part < 3:
                total[rows, :] += value
            else:
                value = ((total[rows, :] + value) * (4096 ** -0.5)).astype(jnp.bfloat16)
                product[wave, px, 0, rows, :] = value[:, :LANES]
                product[wave, px, 1, rows, :] = value[:, LANES:]

    stores = []

    def store(src, dst, index):
        copy = pltpu.make_async_copy(src, dst, store_sem.at[index])
        copy.start()
        stores.append(copy)

    def finish_columns(wave, px):
        for h in range(2):
            o = px * 2 + h
            cols = slice(o * 256 + wave * LANES, o * 256 + (wave + 1) * LANES)
            store(product.at[wave, px, h], kv_out.at[:, cols], 3 + (wave * 4 + px) * 2 + h)

    def own_rows(wave):
        for o in range(NX * 2):
            cols = slice(o * 256 + wave * LANES, o * 256 + (wave + 1) * LANES)
            rounded = tiles[wave, o // 2, (o % 2) * 2 + yl, z, core].astype(jnp.float32)
            exact = slow_new[:, wave * LANES:(wave + 1) * LANES]
            fast_new[:, cols] = jnp.where(jnp.full((128, LANES), o, jnp.int32) == outer, exact, rounded)

    def wave_done(wave):
        ref = tiles.at[wave, :, :, :, other]
        pltpu.make_async_remote_copy(
            src_ref=ref, dst_ref=ref, send_sem=pair_send.at[wave], recv_sem=pair_recv.at[wave],
            device_id=partner, device_id_type=MESH).wait_recv()

    loads[4].wait()
    norm_rows(0, 16)
    remaining = {0: 0, 1: 0}
    for event in PLAN:
        if event[1] == "recv":
            remaining[event[2]] += 1
    work = []
    for number, (now, kind, wave, got, actions, local, index) in enumerate(PLAN):
        if kind == "ready":
            rs_wait(wave)
            update(wave)
        else:
            ref = slice_of(got)
            pltpu.make_async_remote_copy(
                src_ref=ref, dst_ref=ref, send_sem=ag_send.at[0, 0, 0], recv_sem=ag_recv.at[index],
                device_id=partner, device_id_type=MESH).wait_recv()
        for action in actions:
            ag_copy(*action).start()
        for piece in local:
            pair_copy(slice_of(piece), wave).start()
        if kind == "ready":
            norm_rows(16 + 16 * wave, 16)
            if wave == 1:
                store(slow_new, slow_out, 0)
                store(moment_new, moment_out, 1)
            continue
        remaining[wave] -= 1
        if remaining[wave] == 0:
            if wave == 0:
                wave_done(0)
                for px in range(NX):
                    for part in range(4):
                        work.append((px, part))
            else:
                while work:
                    px, part = work.pop(0)
                    matmul(0, px, part)
                    if part == 3:
                        finish_columns(0, px)
                own_rows(0)
                own_rows(1)
                store(fast_new, fast_out, 2)
                wave_done(1)
                for px in range(NX):
                    for part in range(4):
                        matmul(1, px, part)
                    finish_columns(1, px)
        elif work:
            px, part = work.pop(0)
            matmul(0, px, part)
            if part == 3:
                finish_columns(0, px)

    for copy in stores:
        copy.wait()
    for wave in range(WAVES):
        sent = incoming.at[wave, 0:7]
        pltpu.make_async_remote_copy(
            src_ref=sent, dst_ref=sent, send_sem=rs_send.at[wave], recv_sem=rs_recv.at[wave],
            device_id=partner, device_id_type=MESH).wait_send()
        sent = tiles.at[wave, :, :, :, core]
        pltpu.make_async_remote_copy(
            src_ref=sent, dst_ref=sent, send_sem=pair_send.at[wave], recv_sem=pair_recv.at[wave],
            device_id=partner, device_id_type=MESH).wait_send()
        for colour, (axes, *_r) in enumerate(COLOURS):
            lo, hi = COLOURS[colour][1 + wave]
            a, b, c = axes
            ranges = (
                {a: slice(0, SIZES[a] - 1), b: 0, c: 0},
                {a: slice(0, SIZES[a]), b: slice(0, SIZES[b] - 1), c: 0},
                {a: slice(0, SIZES[a]), b: slice(0, SIZES[b]), c: slice(0, SIZES[c] - 1)},
            )
            for phase, span in enumerate(ranges):
                sent = tiles.at[wave, span["x"], span["y"], span["z"], core, lo:hi, :]
                pltpu.make_async_remote_copy(
                    src_ref=sent, dst_ref=sent, send_sem=ag_send.at[wave, colour, phase], recv_sem=ag_recv.at[0],
                    device_id=partner, device_id_type=MESH).wait_send()


def body(fast_weights, slow_weights, momentum, tokens, norm_gain):
    rows, cols = slow_weights.shape
    count, width = tokens.shape
    whole = fast_weights.shape[2]
    hbm = pl.BlockSpec(memory_space=pl.ANY)
    dma = pltpu.SemaphoreType.DMA
    return pl.pallas_call(
        kernel,
        out_shape=(
            jax.ShapeDtypeStruct((rows, cols), jnp.float32),
            jax.ShapeDtypeStruct((rows, cols), jnp.float32),
            jax.ShapeDtypeStruct((rows, whole), jnp.float32),
            jax.ShapeDtypeStruct((count, whole), jnp.bfloat16),
        ),
        in_specs=[hbm] * 5,
        out_specs=(hbm,) * 4,
        scratch_shapes=[
            pltpu.VMEM((WAVES, NX, NY, NZ, 2, 128, LANES), jnp.bfloat16),
            pltpu.VMEM((rows, whole), jnp.float32),
            pltpu.VMEM((WAVES, 8, rows, LANES), jnp.bfloat16),
            pltpu.VMEM((WAVES, 8, rows, LANES), jnp.bfloat16),
            pltpu.VMEM((rows, cols), jnp.float32),
            pltpu.VMEM((rows, cols), jnp.float32),
            pltpu.VMEM((count, width), jnp.bfloat16),
            pltpu.VMEM((1, width), jnp.float32),
            pltpu.VMEM((rows, cols), jnp.float32),
            pltpu.VMEM((rows, cols), jnp.float32),
            pltpu.VMEM((rows, whole), jnp.float32),
            pltpu.VMEM((count, 256), jnp.float32),
            pltpu.VMEM((WAVES, NX, 2, count, LANES), jnp.bfloat16),
            dma((5,)),
            dma((19,)),
            dma((WAVES,)),
            dma((WAVES,)),
            dma((WAVES, 3, 3)),
            dma((COPIES,)),
            dma((WAVES,)),
            dma((WAVES,)),
        ],
        compiler_params=pltpu.CompilerParams(collective_id=0, has_side_effects=True, vmem_limit_bytes=60 * 1024 * 1024),
    )(fast_weights, slow_weights, momentum, tokens, norm_gain.reshape(1, width))


def solution(mesh):
    in_specs = (
        P("outer", "dp", None),
        P("dp", "outer"),
        P("dp", "outer"),
        P(("outer", "dp"), None),
        P(),
    )
    out_specs = (P("dp", "outer"), P("dp", "outer"), P("dp", None), P(("outer", "dp"), None))
    return jax.shard_map(body, mesh=mesh, in_specs=in_specs, out_specs=out_specs, check_vma=False)
```

```python
import heapq

import jax
import jax.numpy as jnp
from jax import lax
from jax.experimental import pallas as pl
from jax.experimental.pallas import tpu as pltpu
from jax.sharding import PartitionSpec as P

OUTER_LR = 0.7
MOMENTUM_COEF = 0.9
EPSILON = 1e-05
MESH = pl.DeviceIdType.MESH

NX, NY, NZ = 4, 4, 8
SIZES = dict(x=NX, y=NY, z=NZ)
WAVES = 2
STEPS = 1
LANES = 128
COLOURS = (
    (("x", "y", "z"), (0, 48), (0, 32)),
    (("z", "y", "x"), (48, 80), (32, 80)),
    (("z", "x", "y"), (80, 128), (80, 128)),
)
MODES = (("dr", "dr", "dr"), ("dr", "dr", "dr"))
LINK = 45.5
HOP, FURTHER = 2.7, 0.75
READY = (0.0, 4.5)
BUSY = 0.0
CHUNK, PAIR = 1.05, 3.0
CHUNKS = [(pair, dy) for dy in (0, 3, 1, 2) for pair in ((0, 1), (3, 2))]


def spans(order, wave, colour):
    lo, hi = COLOURS[colour][1 + wave]
    return hi - lo


class Piece:
    def __init__(self, wave, colour, where):
        self.wave, self.colour, self.where = wave, colour, dict(where)

    def moved(self, axis, step):
        where = dict(self.where)
        where[axis] = (where[axis] - step) % SIZES[axis]
        return Piece(self.wave, self.colour, where)

    def cut(self, axis, half):
        where = dict(self.where)
        lo, hi = where[axis]
        mid = (lo + hi) // 2
        where[axis] = (lo, mid) if half == 0 else (mid, hi)
        return Piece(self.wave, self.colour, where)

    def key(self):
        return (self.wave, self.colour, tuple(sorted(self.where.items())))

    def tiles(self):
        spans = [range(*v) if isinstance(v, tuple) else [v] for v in (self.where[a] for a in "xyz")]
        return [(x, y, z) for x in spans[0] for y in spans[1] for z in spans[2]]

    def kib(self):
        tiles = 1
        for span in self.where.values():
            if isinstance(span, tuple):
                tiles *= span[1] - span[0]
        return tiles * spans(None, self.wave, self.colour) * LANES * 2 / 1024


def make_plan():
    free, heap, order, serial = {(a, s): BUSY for a in "xy" for s in (True, False)}, [], [], [0]
    arrived, missing, core = {}, {}, 0.0
    for wave in range(WAVES):
        for chunk in CHUNKS:
            missing[wave, chunk] = {(c, x, chunk[1], z) for c in range(3) for x in chunk[0] for z in range(NZ)}
    waiting = []
    turn = [(w, c) for w in range(WAVES) for c in CHUNKS]

    def landed(now, wave, piece):
        covered = {(piece.colour, *tile) for tile in piece.tiles()}
        for chunk in CHUNKS:
            left = missing[wave, chunk]
            if left:
                left -= covered
                if not left:
                    waiting.append((now + PAIR, wave, chunk))

    def send(now, actions, piece, axis, step, phase, offset, weight):
        kib, hops, link = piece.kib(), abs(step), (axis, step > 0)
        begin = max(now, free.get(link, 0.0))
        free[link] = begin + kib * hops / LINK
        index = serial[0]
        serial[0] += 1
        actions.append((piece, axis, step, phase, index))
        arrive = begin + kib / LINK + HOP + FURTHER * (hops - 1)
        heapq.heappush(heap, (arrive, index, piece.moved(axis, step), axis, phase, step, offset, weight))

    def start(now, actions, piece, axis, phase):
        far = SIZES[axis] // 2
        direct = phase < 3 and MODES[piece.wave][piece.colour][phase - 1] == "d"
        if not direct:
            for sign in (1, -1):
                send(now, actions, piece, axis, sign, phase, sign, 2)
            return
        for distance in range(1, far):
            for sign in (1, -1):
                send(now, actions, piece, axis, sign * distance, phase, sign * distance, 2)
        if phase == 1:
            sign = 1 if (piece.wave + piece.colour) % 2 else -1
            send(now, actions, piece, axis, sign * far, phase, far, 2)
        else:
            for half, sign in enumerate((1, -1)):
                send(now, actions, piece.cut(COLOURS[piece.colour][0][0], half), axis, sign * far, phase, far, 1)

    def forward(now, actions, got, axis, phase, offset, weight):
        if weight == 1 or (phase < 3 and MODES[got.wave][got.colour][phase - 1] == "d"):
            return
        far, distance, sign = SIZES[axis] // 2, abs(offset), 1 if offset > 0 else -1
        if distance < far - 1:
            send(now, actions, got, axis, sign, phase, offset + sign, 2)
        elif distance == far - 1:
            if phase == 1:
                if sign == (1 if (got.wave + got.colour) % 2 else -1):
                    send(now, actions, got, axis, sign, phase, far, 2)
            else:
                part = got.cut(COLOURS[got.colour][0][0], 0 if sign == 1 else 1)
                send(now, actions, part, axis, sign, phase, far, 1)

    for wave in range(WAVES):
        heapq.heappush(heap, (READY[wave], -9 + wave, None, None, 0, wave, None, None))
    while heap:
        waiting.sort(key=lambda w: (w[1], CHUNKS.index(w[2])))
        ripe = [w for w in waiting if max(w[0], core) <= heap[0][0] and turn[0] == w[1:]]
        if ripe:
            waiting.remove(ripe[0])
            turn.pop(0)
            order.append((max(ripe[0][0], core), "product", ripe[0][1], ripe[0][2], None, None, None))
            core = max(ripe[0][0], core) + CHUNK
            continue
        now, index, got, axis, phase, step, offset, weight = heapq.heappop(heap)
        now = max(now, core)
        actions, local = [], []
        if phase == 0:
            wave = step
            for colour in range(3):
                start(now, actions, Piece(wave, colour, dict(x=0, y=0, z=0)), COLOURS[colour][0][0], 1)
            order.append((now, "ready", wave, None, actions, local, None))
            continue
        wave, colour = got.wave, got.colour
        a, b, c = COLOURS[colour][0]
        forward(now, actions, got, axis, phase, offset, weight)
        if phase == 1:
            tag = (wave, colour)
            arrived[tag] = arrived.get(tag, 0) + 1
            if arrived[tag] == SIZES[a] - 1:
                line = Piece(wave, colour, {a: (0, SIZES[a]), b: 0, c: 0})
                start(now, actions, line, b, 2)
                start(now, actions, line, c, 3)
                local.append(line)
        else:
            full = Piece(wave, colour, {**got.where, a: (0, SIZES[a])})
            tag = (phase, full.key())
            arrived[tag] = arrived.get(tag, 0) + weight
            if arrived[tag] == 2:
                if phase == 2:
                    start(now, actions, full, c, 3)
                local.append(full)
        for piece in local:
            landed(now, wave, piece)
        order.append((now, "recv", wave, got, actions, local, index))
    for time, wave, chunk in sorted(waiting, key=lambda w: (w[1], CHUNKS.index(w[2]))):
        core = max(core, now, time) + CHUNK
        order.append((core, "product", wave, chunk, None, None, None))
    return order, serial[0]


PLAN, COPIES = make_plan()
PAIRS = [piece for event in PLAN if event[1] == "recv" for piece in event[5]]
PAIR_INDEX = {piece.key(): index for index, piece in enumerate(PAIRS)}


def kernel(fast_in, slow_in, moment_in, tokens_in, gain_in,
           slow_new, moment_new, fast_new, key_values,
           tiles, fast, outgoing, incoming, slow, moment, tokens, gain, total,
           load_sem, rs_send, rs_recv, ag_send, ag_recv, pair_send, pair_recv):
    outer, dp = lax.axis_index("outer"), lax.axis_index("dp")
    x, yh = outer // 2, outer % 2
    yl, z, core = dp // 16, (dp // 2) % NZ, dp % 2
    y = yh * 2 + yl
    here = dict(x=x, y=y, z=z)
    other = 1 - core

    def device(px, py, pz, pc):
        return (px * 2 + py // 2, (py % 2) * 16 + pz * 2 + pc)

    def beside(axis, step):
        at = dict(here)
        at[axis] = lax.rem(at[axis] + (step % SIZES[axis]), SIZES[axis])
        return device(at["x"], at["y"], at["z"], core)

    partner = device(x, y, z, other)

    loads = [
        pltpu.make_async_copy(fast_in.at[0], fast, load_sem.at[0]),
        pltpu.make_async_copy(slow_in, slow, load_sem.at[1]),
        pltpu.make_async_copy(moment_in, moment, load_sem.at[2]),
        pltpu.make_async_copy(gain_in, gain, load_sem.at[3]),
        pltpu.make_async_copy(tokens_in, tokens, load_sem.at[4]),
    ]
    for load in loads:
        load.start()

    peers = []
    for dx in range(NX):
        for dy in (0, 2):
            if dx or dy:
                peers.append(device(lax.rem(x + dx, NX), lax.rem(y + dy, NY), z, core))
    greet = list(peers) + [partner, beside("y", 1), beside("y", -1)] + [beside("z", s) for s in range(1, NZ)]
    barrier = pltpu.get_barrier_semaphore()
    for peer in greet:
        pl.semaphore_signal(barrier, inc=1, device_id=peer, device_id_type=MESH)

    loads[0].wait()
    for wave in range(WAVES):
        for o in range(NX * 2):
            outgoing[wave, o] = fast[:, o * 256 + wave * LANES:o * 256 + (wave + 1) * LANES].astype(jnp.bfloat16)
    loads[1].wait()
    loads[2].wait()
    loads[3].wait()
    pl.semaphore_wait(barrier, len(greet))

    for wave in range(WAVES):
        for index, peer in enumerate(peers):
            pltpu.make_async_remote_copy(
                src_ref=outgoing.at[wave, peer[0]], dst_ref=incoming.at[wave, outer],
                send_sem=rs_send.at[wave], recv_sem=rs_recv.at[wave], device_id=peer, device_id_type=MESH).start()

    def norm_rows(first, count):
        @pl.loop(first, first + count)
        def _(i):
            rows = pl.ds(i * 16, 16)
            values = tokens[rows, :].astype(jnp.float32)
            meansq = jnp.mean(values * values, axis=-1, keepdims=True)
            tokens[rows, :] = (values * lax.rsqrt(meansq + EPSILON) * gain[...]).astype(jnp.bfloat16)

    def rs_wait(wave):
        landed = incoming.at[wave, 0:7]
        pltpu.make_async_remote_copy(
            src_ref=landed, dst_ref=landed, send_sem=rs_send.at[wave], recv_sem=rs_recv.at[wave],
            device_id=partner, device_id_type=MESH).wait_recv()

    def update(wave):
        cols = slice(wave * LANES, (wave + 1) * LANES)
        summed = fast[:, pl.ds(pl.multiple_of(outer * 256 + wave * LANES, LANES), LANES)]
        for k in range(1, NX * 2):
            summed = summed + incoming[wave, lax.rem(outer + k, NX * 2)].astype(jnp.float32)
        part = slow[:, cols]
        outer_grad = part - summed / (NX * 2)
        moment_next = MOMENTUM_COEF * moment[:, cols] + outer_grad
        slow_next = part - OUTER_LR * (outer_grad + MOMENTUM_COEF * moment_next)
        tiles[wave, x, y, z, core] = slow_next.astype(jnp.bfloat16)
        slow_new[:, cols] = slow_next
        moment_new[:, cols] = moment_next

    def slice_of(piece, parity):
        lo, hi = COLOURS[piece.colour][1 + piece.wave]
        index = [piece.wave]
        for axis in ("x", "y", "z"):
            span = piece.where[axis]
            if isinstance(span, tuple):
                index.append(slice(span[0], span[1]))
            else:
                index.append(lax.rem(here[axis] + span, SIZES[axis]) if span else here[axis])
        return tiles.at[(*index, parity, slice(lo, hi), slice(None))]

    def ag_copy(piece, axis, step, phase, index):
        ref = slice_of(piece, core)
        return pltpu.make_async_remote_copy(
            src_ref=ref, dst_ref=ref, send_sem=ag_send.at[piece.wave, piece.colour, phase - 1], recv_sem=ag_recv.at[index],
            device_id=beside(axis, step), device_id_type=MESH)

    def pair_copy(piece, parity):
        ref = slice_of(piece, parity)
        return pltpu.make_async_remote_copy(
            src_ref=ref, dst_ref=ref, send_sem=pair_send.at[piece.wave], recv_sem=pair_recv.at[PAIR_INDEX[piece.key()]],
            device_id=partner, device_id_type=MESH)

    collected = set()

    def collect(wave, needed):
        for piece in PAIRS:
            if piece.wave == wave and piece.key() not in collected and needed & set(piece.tiles()):
                collected.add(piece.key())
                pair_copy(piece, other).wait_recv()

    def matmul(k):
        wave, q = k // len(CHUNKS), k % len(CHUNKS)
        turn, pair = q // 2, q % 2
        dy = jnp.where(turn == 0, 0, jnp.where(turn == 1, 3, jnp.where(turn == 2, 1, 2)))
        py = lax.rem(y + dy, NY)
        half = py // 2
        pxs = [lax.rem(x + dx, NX) for dx in (3 * pair, 1 + pair)]
        deep = pl.ds(pl.multiple_of((py % 2) * 2048, 2048), 2048)

        def each(m):
            rows = pl.ds(pl.multiple_of(m * (768 // STEPS), 768 // STEPS), 768 // STEPS)
            weights = jnp.concatenate([tiles[wave, px, py].reshape(2048, LANES) for px in pxs], axis=1)
            total[pair, half, rows] += jnp.dot(tokens[rows, deep], weights, preferred_element_type=jnp.float32)

        if STEPS == 1:
            each(0)
        else:
            pl.loop(0, STEPS)(each)

        @pl.when(turn >= 2)
        def _():
            full = jnp.where(turn == 2, yh, 1 - yh)

            @pl.loop(0, 6)
            def _(m):
                rows = pl.ds(pl.multiple_of(m * 128, 128), 128)
                value = (total[pair, full, rows] * (4096 ** -0.5)).astype(jnp.bfloat16)
                total[pair, full, rows] = jnp.zeros((128, 256), jnp.float32)
                for side, px in enumerate(pxs):
                    first = pl.multiple_of((px * 2 + full) * 256 + wave * LANES, LANES)
                    key_values[rows, pl.ds(first, LANES)] = value[:, side * LANES:(side + 1) * LANES]

    def own_rows(wave):
        for o in range(NX * 2):
            cols = slice(o * 256 + wave * LANES, o * 256 + (wave + 1) * LANES)
            rounded = tiles[wave, o // 2, (o % 2) * 2 + yl, z, core].astype(jnp.float32)
            exact = slow_new[:, wave * LANES:(wave + 1) * LANES]
            fast_new[:, cols] = jnp.where(jnp.full((128, LANES), o, jnp.int32) == outer, exact, rounded)

    total[...] = jnp.zeros_like(total)
    loads[4].wait()
    norm_rows(0, 16)
    def step(event):
        now, kind, wave, got, actions, local, index = event
        if kind == "ready":
            rs_wait(wave)
            update(wave)
        else:
            ref = slice_of(got, core)
            pltpu.make_async_remote_copy(
                src_ref=ref, dst_ref=ref, send_sem=ag_send.at[0, 0, 0], recv_sem=ag_recv.at[index],
                device_id=partner, device_id_type=MESH).wait_recv()
        for action in actions:
            ag_copy(*action).start()
        for piece in local:
            pair_copy(piece, core).start()
        if kind == "ready":
            norm_rows(16 + 16 * wave, 16)

    groups = [[]]
    for event in PLAN:
        groups[-1].append(event)
        if event[1] == "product":
            groups.append([])
    for event in groups[0][:-1]:
        step(event)
    groups[0] = groups[0][-1:]

    @pl.loop(0, 2 * len(CHUNKS))
    def _(k):
        for number, group in enumerate(groups[:-1]):
            @pl.when(k == number)
            def _():
                for event in group[:-1]:
                    step(event)
                wave, (pair, dy) = group[-1][2:4]
                if number in (len(CHUNKS), 2 * len(CHUNKS) - 1):
                    own_rows(number // len(CHUNKS) - 1 if number == len(CHUNKS) else 1)
                collect(wave, {(dx, dy, dz) for dx in pair for dz in range(NZ)})

        matmul(k)

    for wave in range(WAVES):
        sent = incoming.at[wave, 0:7]
        pltpu.make_async_remote_copy(
            src_ref=sent, dst_ref=sent, send_sem=rs_send.at[wave], recv_sem=rs_recv.at[wave],
            device_id=partner, device_id_type=MESH).wait_send()
        sent = tiles.at[wave, :, :, :, core]
        pltpu.make_async_remote_copy(
            src_ref=sent, dst_ref=sent, send_sem=pair_send.at[wave], recv_sem=pair_recv.at[0],
            device_id=partner, device_id_type=MESH).wait_send()
        for colour, (axes, *_r) in enumerate(COLOURS):
            lo, hi = COLOURS[colour][1 + wave]
            a, b, c = axes
            ranges = (
                {a: slice(0, SIZES[a] - 1), b: 0, c: 0},
                {a: slice(0, SIZES[a]), b: slice(0, SIZES[b] - 1), c: 0},
                {a: slice(0, SIZES[a]), b: slice(0, SIZES[b]), c: slice(0, SIZES[c] - 1)},
            )
            for phase, span in enumerate(ranges):
                sent = tiles.at[wave, span["x"], span["y"], span["z"], core, lo:hi, :]
                pltpu.make_async_remote_copy(
                    src_ref=sent, dst_ref=sent, send_sem=ag_send.at[wave, colour, phase], recv_sem=ag_recv.at[0],
                    device_id=partner, device_id_type=MESH).wait_send()


def keep(slow_new, moment_new, fast_new, key_values, slow_out, moment_out, fast_out, kv_out, sem):
    copies = []
    count = key_values.shape[0]
    for q in range(4):
        rows = slice(q * count // 4, (q + 1) * count // 4)
        copies.append(pltpu.make_async_copy(key_values.at[rows], kv_out.at[rows], sem.at[q]))
    copies.append(pltpu.make_async_copy(fast_new, fast_out, sem.at[4]))
    copies.append(pltpu.make_async_copy(slow_new, slow_out, sem.at[5]))
    copies.append(pltpu.make_async_copy(moment_new, moment_out, sem.at[6]))
    for copy in copies:
        copy.start()
    for copy in copies:
        copy.wait()


def body(fast_weights, slow_weights, momentum, tokens, norm_gain):
    rows, cols = slow_weights.shape
    count, width = tokens.shape
    whole = fast_weights.shape[2]
    hbm = pl.BlockSpec(memory_space=pltpu.HBM)
    dma = pltpu.SemaphoreType.DMA
    made = pl.pallas_call(
        kernel,
        out_shape=(
            jax.ShapeDtypeStruct((rows, cols), jnp.float32),
            jax.ShapeDtypeStruct((rows, cols), jnp.float32),
            jax.ShapeDtypeStruct((rows, whole), jnp.float32),
            jax.ShapeDtypeStruct((count, whole), jnp.bfloat16),
        ),
        in_specs=[hbm] * 5,
        out_specs=(pl.BlockSpec(memory_space=pltpu.VMEM),) * 4,
        scratch_shapes=[
            pltpu.VMEM((WAVES, NX, NY, NZ, 2, 128, LANES), jnp.bfloat16),
            pltpu.VMEM((rows, whole), jnp.float32),
            pltpu.VMEM((WAVES, 8, rows, LANES), jnp.bfloat16),
            pltpu.VMEM((WAVES, 8, rows, LANES), jnp.bfloat16),
            pltpu.VMEM((rows, cols), jnp.float32),
            pltpu.VMEM((rows, cols), jnp.float32),
            pltpu.VMEM((count, width), jnp.bfloat16),
            pltpu.VMEM((1, width), jnp.float32),
            pltpu.VMEM((2, 2, count, 256), jnp.float32),
            dma((5,)),
            dma((WAVES,)),
            dma((WAVES,)),
            dma((WAVES, 3, 3)),
            dma((COPIES,)),
            dma((WAVES,)),
            dma((len(PAIRS),)),
        ],
        compiler_params=pltpu.CompilerParams(collective_id=0, has_side_effects=True, vmem_limit_bytes=48 * 1024 * 1024),
    )(fast_weights, slow_weights, momentum, tokens, norm_gain.reshape(1, width))
    return pl.pallas_call(
        keep,
        out_shape=tuple(jax.ShapeDtypeStruct(m.shape, m.dtype) for m in made),
        in_specs=[pl.BlockSpec(memory_space=pl.ANY)] * 4,
        out_specs=(hbm,) * 4,
        scratch_shapes=[dma((8,))],
        compiler_params=pltpu.CompilerParams(vmem_limit_bytes=1024 * 1024),
    )(*made)


def solution(mesh):
    in_specs = (
        P("outer", "dp", None),
        P("dp", "outer"),
        P("dp", "outer"),
        P(("outer", "dp"), None),
        P(),
    )
    out_specs = (P("dp", "outer"), P("dp", "outer"), P("dp", None), P(("outer", "dp"), None))
    return jax.shard_map(body, mesh=mesh, in_specs=in_specs, out_specs=out_specs, check_vma=False)
```

```python
import heapq

import jax
import jax.numpy as jnp
from jax import lax
from jax.experimental import pallas as pl
from jax.experimental.pallas import tpu as pltpu
from jax.sharding import PartitionSpec as P

OUTER_LR = 0.7
MOMENTUM_COEF = 0.9
EPSILON = 1e-05
MESH = pl.DeviceIdType.MESH

NX, NY, NZ = 4, 4, 8
SIZES = dict(x=NX, y=NY, z=NZ)
WAVES = 2
STEPS = 1
LANES = 128
COLOURS = (
    (("x", "y", "z"), (0, 48), (0, 32)),
    (("z", "x", "y"), (48, 80), (32, 96)),
    (("z", "y", "x"), (80, 128), (96, 128)),
)
MODES = (("dr", "dr", "dr"), ("rr", "dr", "dr"))
LINK = 45.5
HOP, FURTHER = 2.7, 0.75
READY = (0.0, 4.5)
BUSY = 0.0
CHUNK, PAIR = 1.05, 3.0
CHUNKS = [(pair, dy) for dy in (0, 3, 1, 2) for pair in ((0, 1), (3, 2))]


def spans(order, wave, colour):
    lo, hi = COLOURS[colour][1 + wave]
    return hi - lo


class Piece:
    def __init__(self, wave, colour, where):
        self.wave, self.colour, self.where = wave, colour, dict(where)

    def moved(self, axis, step):
        where = dict(self.where)
        where[axis] = (where[axis] - step) % SIZES[axis]
        return Piece(self.wave, self.colour, where)

    def cut(self, axis, half):
        where = dict(self.where)
        lo, hi = where[axis]
        mid = (lo + hi) // 2
        where[axis] = (lo, mid) if half == 0 else (mid, hi)
        return Piece(self.wave, self.colour, where)

    def key(self):
        return (self.wave, self.colour, tuple(sorted(self.where.items())))

    def tiles(self):
        spans = [range(*v) if isinstance(v, tuple) else [v] for v in (self.where[a] for a in "xyz")]
        return [(x, y, z) for x in spans[0] for y in spans[1] for z in spans[2]]

    def kib(self):
        tiles = 1
        for span in self.where.values():
            if isinstance(span, tuple):
                tiles *= span[1] - span[0]
        return tiles * spans(None, self.wave, self.colour) * LANES * 2 / 1024


def make_plan():
    free, heap, order, serial = {(a, s): BUSY for a in "xy" for s in (True, False)}, [], [], [0]
    arrived, missing, core = {}, {}, 0.0
    for wave in range(WAVES):
        for chunk in CHUNKS:
            missing[wave, chunk] = {(c, x, chunk[1], z) for c in range(3) for x in chunk[0] for z in range(NZ)}
    waiting = []
    turn = [(w, c) for w in range(WAVES) for c in CHUNKS]

    def landed(now, wave, piece):
        covered = {(piece.colour, *tile) for tile in piece.tiles()}
        for chunk in CHUNKS:
            left = missing[wave, chunk]
            if left:
                left -= covered
                if not left:
                    waiting.append((now + PAIR, wave, chunk))

    def send(now, actions, piece, axis, step, phase, offset, weight):
        kib, hops, link = piece.kib(), abs(step), (axis, step > 0)
        begin = max(now, free.get(link, 0.0))
        free[link] = begin + kib * hops / LINK
        index = serial[0]
        serial[0] += 1
        actions.append((piece, axis, step, phase, index))
        arrive = begin + kib / LINK + HOP + FURTHER * (hops - 1)
        heapq.heappush(heap, (arrive, index, piece.moved(axis, step), axis, phase, step, offset, weight))

    def start(now, actions, piece, axis, phase):
        far = SIZES[axis] // 2
        direct = phase < 3 and MODES[piece.wave][piece.colour][phase - 1] == "d"
        if not direct:
            for sign in (1, -1):
                send(now, actions, piece, axis, sign, phase, sign, 2)
            return
        for distance in range(1, far):
            for sign in (1, -1):
                send(now, actions, piece, axis, sign * distance, phase, sign * distance, 2)
        if phase == 1:
            sign = 1 if (piece.wave + piece.colour) % 2 else -1
            send(now, actions, piece, axis, sign * far, phase, far, 2)
        else:
            for half, sign in enumerate((1, -1)):
                send(now, actions, piece.cut(COLOURS[piece.colour][0][0], half), axis, sign * far, phase, far, 1)

    def forward(now, actions, got, axis, phase, offset, weight):
        if weight == 1 or (phase < 3 and MODES[got.wave][got.colour][phase - 1] == "d"):
            return
        far, distance, sign = SIZES[axis] // 2, abs(offset), 1 if offset > 0 else -1
        if distance < far - 1:
            send(now, actions, got, axis, sign, phase, offset + sign, 2)
        elif distance == far - 1:
            if phase == 1:
                if sign == (1 if (got.wave + got.colour) % 2 else -1):
                    send(now, actions, got, axis, sign, phase, far, 2)
            else:
                part = got.cut(COLOURS[got.colour][0][0], 0 if sign == 1 else 1)
                send(now, actions, part, axis, sign, phase, far, 1)

    for wave in range(WAVES):
        heapq.heappush(heap, (READY[wave], -9 + wave, None, None, 0, wave, None, None))
    while heap:
        waiting.sort(key=lambda w: (w[1], CHUNKS.index(w[2])))
        ripe = [w for w in waiting if max(w[0], core) <= heap[0][0] and turn[0] == w[1:]]
        if ripe:
            waiting.remove(ripe[0])
            turn.pop(0)
            order.append((max(ripe[0][0], core), "product", ripe[0][1], ripe[0][2], None, None, None))
            core = max(ripe[0][0], core) + CHUNK
            continue
        now, index, got, axis, phase, step, offset, weight = heapq.heappop(heap)
        now = max(now, core)
        actions, local = [], []
        if phase == 0:
            wave = step
            for colour in range(3):
                start(now, actions, Piece(wave, colour, dict(x=0, y=0, z=0)), COLOURS[colour][0][0], 1)
            order.append((now, "ready", wave, None, actions, local, None))
            continue
        wave, colour = got.wave, got.colour
        a, b, c = COLOURS[colour][0]
        forward(now, actions, got, axis, phase, offset, weight)
        if phase == 1:
            tag = (wave, colour)
            arrived[tag] = arrived.get(tag, 0) + 1
            if arrived[tag] == SIZES[a] - 1:
                line = Piece(wave, colour, {a: (0, SIZES[a]), b: 0, c: 0})
                start(now, actions, line, b, 2)
                start(now, actions, line, c, 3)
                local.append(line)
        else:
            full = Piece(wave, colour, {**got.where, a: (0, SIZES[a])})
            tag = (phase, full.key())
            arrived[tag] = arrived.get(tag, 0) + weight
            if arrived[tag] == 2:
                if phase == 2:
                    start(now, actions, full, c, 3)
                local.append(full)
        for piece in local:
            landed(now, wave, piece)
        order.append((now, "recv", wave, got, actions, local, index))
    for time, wave, chunk in sorted(waiting, key=lambda w: (w[1], CHUNKS.index(w[2]))):
        core = max(core, now, time) + CHUNK
        order.append((core, "product", wave, chunk, None, None, None))
    return order, serial[0]


PLAN, COPIES = make_plan()
PAIRS = [piece for event in PLAN if event[1] == "recv" for piece in event[5]]
PAIR_INDEX = {piece.key(): index for index, piece in enumerate(PAIRS)}


def kernel(fast, packed, tokens_in,
           slow_new, moment_new, fast_new, key_values,
           tiles, outgoing, incoming, tokens, gain, total,
           load_sem, rs_send, rs_recv, ag_send, ag_recv, pair_send, pair_recv):
    outer, dp = lax.axis_index("outer"), lax.axis_index("dp")
    x, yh = outer // 2, outer % 2
    yl, z, core = dp // 16, (dp // 2) % NZ, dp % 2
    y = yh * 2 + yl
    here = dict(x=x, y=y, z=z)
    other = 1 - core

    def device(px, py, pz, pc):
        return (px * 2 + py // 2, (py % 2) * 16 + pz * 2 + pc)

    def beside(axis, step):
        at = dict(here)
        at[axis] = lax.rem(at[axis] + (step % SIZES[axis]), SIZES[axis])
        return device(at["x"], at["y"], at["z"], core)

    partner = device(x, y, z, other)

    load = pltpu.make_async_copy(tokens_in, tokens, load_sem.at[0])
    load.start()
    deep, wide = 128, 256
    slow, moment = packed.at[0:deep], packed.at[deep:2 * deep]
    for r in range(4096 // wide):
        gain[0:1, r * wide:(r + 1) * wide] = packed[2 * deep + r:2 * deep + r + 1, :]

    peers = []
    for dx in range(NX):
        for dy in (0, 2):
            if dx or dy:
                peers.append(device(lax.rem(x + dx, NX), lax.rem(y + dy, NY), z, core))
    greet = list(peers) + [partner, beside("y", 1), beside("y", -1)] + [beside("z", s) for s in range(1, NZ)]
    barrier = pltpu.get_barrier_semaphore()
    for peer in greet:
        pl.semaphore_signal(barrier, inc=1, device_id=peer, device_id_type=MESH)

    for wave in range(WAVES):
        @pl.loop(0, NX * 2)
        def _(o):
            cols = pl.ds(pl.multiple_of(o * 256 + wave * LANES, LANES), LANES)
            outgoing[wave, o] = fast[0, :, cols].astype(jnp.bfloat16)

        if wave == 0:
            pl.semaphore_wait(barrier, len(greet))
        for index, peer in enumerate(peers):
            pltpu.make_async_remote_copy(
                src_ref=outgoing.at[wave, peer[0]], dst_ref=incoming.at[wave, outer],
                send_sem=rs_send.at[wave], recv_sem=rs_recv.at[wave], device_id=peer, device_id_type=MESH).start()

    def norm_rows(first, count):
        @pl.loop(first, first + count)
        def _(i):
            rows = pl.ds(i * 16, 16)
            values = tokens[rows, :].astype(jnp.float32)
            meansq = jnp.mean(values * values, axis=-1, keepdims=True)
            tokens[rows, :] = (values * lax.rsqrt(meansq + EPSILON) * gain[...]).astype(jnp.bfloat16)

    def rs_wait(wave):
        landed = incoming.at[wave, 0:7]
        pltpu.make_async_remote_copy(
            src_ref=landed, dst_ref=landed, send_sem=rs_send.at[wave], recv_sem=rs_recv.at[wave],
            device_id=partner, device_id_type=MESH).wait_recv()

    def update(wave):
        cols = slice(wave * LANES, (wave + 1) * LANES)
        summed = fast[0, :, pl.ds(pl.multiple_of(outer * 256 + wave * LANES, LANES), LANES)]
        for k in range(1, NX * 2):
            summed = summed + incoming[wave, lax.rem(outer + k, NX * 2)].astype(jnp.float32)
        part = slow[:, cols]
        outer_grad = part - summed / (NX * 2)
        moment_next = MOMENTUM_COEF * moment[:, cols] + outer_grad
        slow_next = part - OUTER_LR * (outer_grad + MOMENTUM_COEF * moment_next)
        tiles[wave, x, y, z, core] = slow_next.astype(jnp.bfloat16)
        slow_new[:, cols] = slow_next
        moment_new[:, cols] = moment_next

    def slice_of(piece, parity):
        lo, hi = COLOURS[piece.colour][1 + piece.wave]
        index = [piece.wave]
        for axis in ("x", "y", "z"):
            span = piece.where[axis]
            if isinstance(span, tuple):
                index.append(slice(span[0], span[1]))
            else:
                index.append(lax.rem(here[axis] + span, SIZES[axis]) if span else here[axis])
        return tiles.at[(*index, parity, slice(lo, hi), slice(None))]

    def ag_copy(piece, axis, step, phase, index):
        ref = slice_of(piece, core)
        return pltpu.make_async_remote_copy(
            src_ref=ref, dst_ref=ref, send_sem=ag_send.at[piece.wave, piece.colour, phase - 1], recv_sem=ag_recv.at[index],
            device_id=beside(axis, step), device_id_type=MESH)

    def pair_copy(piece, parity):
        ref = slice_of(piece, parity)
        return pltpu.make_async_remote_copy(
            src_ref=ref, dst_ref=ref, send_sem=pair_send.at[piece.wave], recv_sem=pair_recv.at[PAIR_INDEX[piece.key()]],
            device_id=partner, device_id_type=MESH)

    collected = set()

    def collect(wave, needed):
        for piece in PAIRS:
            if piece.wave == wave and piece.key() not in collected and needed & set(piece.tiles()):
                collected.add(piece.key())
                pair_copy(piece, other).wait_recv()

    def matmul(k):
        wave, q = k // len(CHUNKS), k % len(CHUNKS)
        turn, pair = q // 2, q % 2
        dy = jnp.where(turn == 0, 0, jnp.where(turn == 1, 3, jnp.where(turn == 2, 1, 2)))
        py = lax.rem(y + dy, NY)
        half = py // 2
        pxs = [lax.rem(x + dx, NX) for dx in (3 * pair, 1 + pair)]
        deep = pl.ds(pl.multiple_of((py % 2) * 2048, 2048), 2048)

        def each(m):
            rows = pl.ds(pl.multiple_of(m * (768 // STEPS), 768 // STEPS), 768 // STEPS)
            weights = jnp.concatenate([tiles[wave, px, py].reshape(2048, LANES) for px in pxs], axis=1)
            total[pair, half, rows] += jnp.dot(tokens[rows, deep], weights, preferred_element_type=jnp.float32)

        if STEPS == 1:
            each(0)
        else:
            pl.loop(0, STEPS)(each)

        @pl.when(turn >= 2)
        def _():
            full = jnp.where(turn == 2, yh, 1 - yh)

            @pl.loop(0, 6)
            def _(m):
                rows = pl.ds(pl.multiple_of(m * 128, 128), 128)
                value = (total[pair, full, rows] * (4096 ** -0.5)).astype(jnp.bfloat16)
                total[pair, full, rows] = jnp.zeros((128, 256), jnp.float32)
                for side, px in enumerate(pxs):
                    first = pl.multiple_of((px * 2 + full) * 256 + wave * LANES, LANES)
                    key_values[rows, pl.ds(first, LANES)] = value[:, side * LANES:(side + 1) * LANES]

    def own_rows(wave):
        @pl.loop(0, NX * 2)
        def _(o):
            cols = pl.ds(pl.multiple_of(o * 256 + wave * LANES, LANES), LANES)
            fast_new[:, cols] = tiles[wave, o // 2, (o % 2) * 2 + yl, z, core].astype(jnp.float32)

        cols = pl.ds(pl.multiple_of(outer * 256 + wave * LANES, LANES), LANES)
        fast_new[:, cols] = slow_new[:, wave * LANES:(wave + 1) * LANES]

    total[...] = jnp.zeros_like(total)
    load.wait()
    norm_rows(0, 16)
    def step(event):
        now, kind, wave, got, actions, local, index = event
        if kind == "ready":
            rs_wait(wave)
            update(wave)
        else:
            ref = slice_of(got, core)
            pltpu.make_async_remote_copy(
                src_ref=ref, dst_ref=ref, send_sem=ag_send.at[0, 0, 0], recv_sem=ag_recv.at[index],
                device_id=partner, device_id_type=MESH).wait_recv()
        for action in actions:
            ag_copy(*action).start()
        for piece in local:
            pair_copy(piece, core).start()
        if kind == "ready":
            norm_rows(16 + 16 * wave, 16)

    groups = [[]]
    for event in PLAN:
        groups[-1].append(event)
        if event[1] == "product":
            groups.append([])
    for event in groups[0][:-1]:
        step(event)
    groups[0] = groups[0][-1:]

    def arrive(number):
        group = groups[number]
        for event in group[:-1]:
            step(event)
        wave, (pair, dy) = group[-1][2:4]
        if number == len(CHUNKS):
            own_rows(0)
        if number == 2 * len(CHUNKS) - 1:
            own_rows(1)
        collect(wave, {(dx, dy, dz) for dx in pair for dz in range(NZ)})

    def branch(k, first, last):
        if last - first == 1:
            arrive(first)
            return
        middle = (first + last) // 2

        @pl.when(k < middle)
        def _():
            branch(k, first, middle)

        @pl.when(k >= middle)
        def _():
            branch(k, middle, last)

    @pl.loop(0, 2 * len(CHUNKS))
    def _(k):
        branch(k, 0, len(groups) - 1)
        matmul(k)

    for wave in range(WAVES):
        sent = incoming.at[wave, 0:7]
        pltpu.make_async_remote_copy(
            src_ref=sent, dst_ref=sent, send_sem=rs_send.at[wave], recv_sem=rs_recv.at[wave],
            device_id=partner, device_id_type=MESH).wait_send()
        sent = tiles.at[wave, :, :, :, core]
        pltpu.make_async_remote_copy(
            src_ref=sent, dst_ref=sent, send_sem=pair_send.at[wave], recv_sem=pair_recv.at[0],
            device_id=partner, device_id_type=MESH).wait_send()
        for colour, (axes, *_r) in enumerate(COLOURS):
            lo, hi = COLOURS[colour][1 + wave]
            a, b, c = axes
            ranges = (
                {a: slice(0, SIZES[a] - 1), b: 0, c: 0},
                {a: slice(0, SIZES[a]), b: slice(0, SIZES[b] - 1), c: 0},
                {a: slice(0, SIZES[a]), b: slice(0, SIZES[b]), c: slice(0, SIZES[c] - 1)},
            )
            for phase, span in enumerate(ranges):
                sent = tiles.at[wave, span["x"], span["y"], span["z"], core, lo:hi, :]
                pltpu.make_async_remote_copy(
                    src_ref=sent, dst_ref=sent, send_sem=ag_send.at[wave, colour, phase], recv_sem=ag_recv.at[0],
                    device_id=partner, device_id_type=MESH).wait_send()


def keep(slow_new, moment_new, fast_new, key_values, slow_out, moment_out, fast_out, kv_out, sem):
    copies = []
    count = key_values.shape[0]
    for q in range(4):
        rows = slice(q * count // 4, (q + 1) * count // 4)
        copies.append(pltpu.make_async_copy(key_values.at[rows], kv_out.at[rows], sem.at[q]))
    copies.append(pltpu.make_async_copy(fast_new, fast_out, sem.at[4]))
    copies.append(pltpu.make_async_copy(slow_new, slow_out, sem.at[5]))
    copies.append(pltpu.make_async_copy(moment_new, moment_out, sem.at[6]))
    for copy in copies:
        copy.start()
    for copy in copies:
        copy.wait()


def body(fast_weights, slow_weights, momentum, tokens, norm_gain):
    rows, cols = slow_weights.shape
    count, width = tokens.shape
    whole = fast_weights.shape[2]
    hbm = pl.BlockSpec(memory_space=pltpu.HBM)
    vmem = pl.BlockSpec(memory_space=pltpu.VMEM)
    dma = pltpu.SemaphoreType.DMA
    packed = jnp.concatenate([slow_weights, momentum, norm_gain.reshape(-1, cols)], axis=0)
    made = pl.pallas_call(
        kernel,
        out_shape=(
            jax.ShapeDtypeStruct((rows, cols), jnp.float32),
            jax.ShapeDtypeStruct((rows, cols), jnp.float32),
            jax.ShapeDtypeStruct((rows, whole), jnp.float32),
            jax.ShapeDtypeStruct((count, whole), jnp.bfloat16),
        ),
        in_specs=[vmem, vmem, hbm],
        out_specs=(pl.BlockSpec(memory_space=pltpu.VMEM),) * 4,
        scratch_shapes=[
            pltpu.VMEM((WAVES, NX, NY, NZ, 2, 128, LANES), jnp.bfloat16),
            pltpu.VMEM((WAVES, 8, rows, LANES), jnp.bfloat16),
            pltpu.VMEM((WAVES, 8, rows, LANES), jnp.bfloat16),
            pltpu.VMEM((count, width), jnp.bfloat16),
            pltpu.VMEM((1, width), jnp.float32),
            pltpu.VMEM((2, 2, count, 256), jnp.float32),
            dma((1,)),
            dma((WAVES,)),
            dma((WAVES,)),
            dma((WAVES, 3, 3)),
            dma((COPIES,)),
            dma((WAVES,)),
            dma((len(PAIRS),)),
        ],
        compiler_params=pltpu.CompilerParams(collective_id=0, has_side_effects=True, vmem_limit_bytes=48 * 1024 * 1024),
    )(fast_weights, packed, tokens)
    return pl.pallas_call(
        keep,
        out_shape=tuple(jax.ShapeDtypeStruct(m.shape, m.dtype) for m in made),
        in_specs=[pl.BlockSpec(memory_space=pl.ANY)] * 4,
        out_specs=(hbm,) * 4,
        scratch_shapes=[dma((8,))],
        compiler_params=pltpu.CompilerParams(vmem_limit_bytes=1024 * 1024),
    )(*made)


def solution(mesh):
    in_specs = (
        P("outer", "dp", None),
        P("dp", "outer"),
        P("dp", "outer"),
        P(("outer", "dp"), None),
        P(),
    )
    out_specs = (P("dp", "outer"), P("dp", "outer"), P("dp", None), P(("outer", "dp"), None))
    return jax.shard_map(body, mesh=mesh, in_specs=in_specs, out_specs=out_specs, check_vma=False)
```
